32 devices in a mesh: energy: 16 (over z, x, core), space: 2 (over y).
Axes of the slice: x: 2, y: 2, z: 4, core: 2. Of those that a mesh axis runs over, the one named last changes fastest.
Arguments:
- g_lesser: float32 [2, 256, 2, 256, 256], P(None, 'energy', 'space'), may hold values from -6 to 6
- g_greater: float32 [2, 256, 2, 256, 256], P(None, 'energy', 'space'), may hold values from -6 to 6
- v_diag: float32 [2, 256, 256], P('space'), may hold values from -0.375 to 0.375
- v_upper: float32 [2, 256, 256], P('space'), may hold values from -0.375 to 0.375
Outputs:
- screened: float32 [2, 64, 2, 256, 256], P(None, 'energy', 'space')
The draws below stay inside these ranges and needn't reach their ends.
All inputs are finite; a program needn't handle non-finite values.
Results may differ from the reference program's by a relative error of at most 0.000098.
Values sent between devices are 32-bit elements; how exact they have to be, the bound alone decides.
A program may use at most 128 MiB of HBM per device.

```python
import math
import jax
import jax.numpy as jnp
from jax import lax

NE = 256
NW = 64
B = 256
NB = 2


def steps_of(rng, shape, shards, smallest, top_value):
    level, own = 1.0, jax.random.fold_in(rng, 6)
    for dim, parts in shards:
        heights = jnp.exp(jax.random.uniform(jax.random.fold_in(own, dim), (parts,), jnp.float32, smallest / len(shards), top_value / len(shards)))
        level = level * jnp.repeat(heights, shape[dim] // parts).reshape([-1 if axis == dim else 1 for axis in range(len(shape))])
    return level


def scatter_about(rng, extent, width, limit, shards=(), kind=jnp.bfloat16):
    drawn = width * jax.random.normal(rng, extent, jnp.float32)
    if shards:
        drawn = drawn * steps_of(rng, extent, shards, -0.22, 0.18)
    return jnp.clip(drawn, -limit, limit).astype(kind)


def setup_inputs(seed: int = 0) -> dict:
    key_of = jax.random.split(jax.random.key(seed), 5)
    return {
        "g_lesser": scatter_about(key_of[0], (2, NE, NB, B, B), 1.0, 6.0, ((1, 16), (2, 2)), jnp.float32),
        "g_greater": scatter_about(key_of[1], (2, NE, NB, B, B), 1.0, 6.0, ((1, 16), (2, 2)), jnp.float32),
        "v_diag": scatter_about(key_of[2], (NB, B, B), B ** -0.5, 0.375, ((0, 2),), jnp.float32),
        "v_upper": scatter_about(key_of[3], (NB, B, B), B ** -0.5, 0.375, ((0, 2),), jnp.float32),
    }


prefactor = 0.0625


def tables(count):
    length = 2 * count
    freqs = jnp.arange(length, dtype=jnp.int32)[:, None]
    points = jnp.arange(count, dtype=jnp.int32)[None, :]
    phase = (2.0 * math.pi / length) * ((freqs * points) % length).astype(jnp.float32)
    return jnp.cos(phase), jnp.sin(phase)


def product(left, right):
    return jnp.dot(left, right, precision=lax.Precision.HIGHEST, preferred_element_type=jnp.float32)


def correlate(lesser, greater, keep):
    count = lesser.shape[1]
    rest = tuple(lesser.shape[2:])
    lesser = lesser.reshape(2, count, -1)
    greater = greater.reshape(2, count, -1)
    cosine, sine = tables(count)
    less_re = product(cosine, lesser[0]) + product(sine, lesser[1])
    less_im = product(cosine, lesser[1]) - product(sine, lesser[0])
    great_re = product(cosine, greater[0]) - product(sine, greater[1])
    great_im = product(cosine, greater[1]) + product(sine, greater[0])
    spec_re = less_re * great_re - less_im * great_im
    spec_im = less_re * great_im + less_im * great_re
    factor = prefactor / (2 * count)
    back_cos = cosine.T[:keep]
    back_sin = sine.T[:keep]
    out_re = (product(back_cos, spec_re) - product(back_sin, spec_im)) * factor
    out_im = (product(back_cos, spec_im) + product(back_sin, spec_re)) * factor
    return jnp.stack([out_re, out_im]).reshape((2, keep) + rest)


def sandwich(left, middle, right):
    halfway = jnp.einsum('rab,...rbd->...rad', left, middle, precision=lax.Precision.HIGHEST)
    return jnp.einsum('...rad,rdf->...raf', halfway, right, precision=lax.Precision.HIGHEST)


def reference(g_lesser, g_greater, v_diag, v_upper):
    flipped = jnp.swapaxes(g_greater, 3, 4)

    def one_row(pair):
        return correlate(pair[0], pair[1], NW)

    rows = lax.map(one_row, (jnp.moveaxis(g_lesser, 2, 0), jnp.moveaxis(flipped, 2, 0)))
    polar = jnp.moveaxis(rows, 0, 2)
    uppers_before = jnp.concatenate([jnp.zeros((1,) + tuple(v_upper.shape[1:]), jnp.float32), v_upper[:-1]], axis=0)
    upper_swapped = jnp.swapaxes(v_upper, 1, 2)
    before_swapped = jnp.swapaxes(uppers_before, 1, 2)

    def one_energy(block):
        padded = jnp.pad(block, ((0, 0), (1, 1), (0, 0), (0, 0)))
        own_term = sandwich(v_diag, block, v_diag)
        above_term = sandwich(before_swapped, padded[:, :-2], uppers_before)
        below_term = sandwich(v_upper, padded[:, 2:], upper_swapped)
        return own_term + above_term + below_term

    result = lax.map(one_energy, jnp.moveaxis(polar, 1, 0))
    return jnp.moveaxis(result, 0, 1)
```

```python
import functools
import math

import jax
import jax.numpy as jnp
import numpy as np
from jax import lax
from jax.experimental import pallas as pl
from jax.experimental.pallas import tpu as pltpu
from jax.sharding import PartitionSpec as P

NW = 64
PREFACTOR = 0.0625
ROWS = 8
LANES = 128
HIGH = lax.Precision.HIGH


def split_np(table):
    table = np.asarray(table, np.float64)
    high = table.astype(jnp.bfloat16)
    low = (table - high.astype(np.float64)).astype(jnp.bfloat16)
    return np.concatenate([high, low, high], axis=1)


def tables(count, keep):
    length = -(-(count + keep) // 64) * 64
    freqs = np.arange(length)[:, None]
    points = np.arange(count)[None, :]
    phase = 2.0 * math.pi / length * (freqs * points % length)
    cos, sin = np.cos(phase), np.sin(phase)
    factor = PREFACTOR / length
    back_cos, back_sin = cos.T[:keep] * factor, sin.T[:keep] * factor
    lesser = np.block([[cos, sin], [-sin, cos]])
    greater = np.block([[cos, -sin], [sin, cos]])
    back = np.block([[back_cos, -back_sin], [back_sin, back_cos]])
    return [jnp.asarray(split_np(t)) for t in (lesser, greater, back)]


def stacked(value):
    high = value.astype(jnp.bfloat16)
    low = (value - high.astype(jnp.float32)).astype(jnp.bfloat16)
    return jnp.concatenate([high, high, low], axis=0)


def dot(table, value):
    return jnp.dot(table, stacked(value), preferred_element_type=jnp.float32)


def correlate_kernel(
    n, lanes_parts, less_tab, great_tab, back_tab, less, great, out,
    less_buf, great_buf, polar_buf, in_send, in_recv, own_sem, out_send, out_recv, out_own,
):
    me = lax.axis_index("energy")
    sources, buffers = (less, great), (less_buf, great_buf)
    held = less.shape[1]
    kept = out.shape[1]
    chunks = less_buf.shape[0]
    count = less_buf.shape[2]
    keep = polar_buf.shape[2]

    def place(c):
        if isinstance(c, int):
            return c // lanes_parts, pl.ds(c % lanes_parts * LANES, LANES)
        return c // lanes_parts, pl.ds(pl.multiple_of(c % lanes_parts * LANES, LANES), LANES)

    def in_copy(k, c, d):
        peer = lax.rem(me + d, n)
        row, lane = place(c)
        return pltpu.make_async_remote_copy(
            src_ref=sources[k].at[:, :, peer, row, :, lane],
            dst_ref=buffers[k].at[c, :, pl.ds(me * held, held)],
            send_sem=in_send.at[k, c, d],
            recv_sem=in_recv.at[k, c, d],
            device_id={"energy": peer},
            device_id_type=pl.DeviceIdType.MESH,
        )

    def in_own(k, c):
        row, lane = place(c)
        return pltpu.make_async_copy(
            sources[k].at[:, :, me, row, :, lane],
            buffers[k].at[c, :, pl.ds(me * held, held)],
            own_sem.at[k, c],
        )

    def out_copy(c, d):
        peer = lax.rem(me + d, n)
        row, lane = place(c)
        return pltpu.make_async_remote_copy(
            src_ref=polar_buf.at[c, :, pl.ds(peer * kept, kept)],
            dst_ref=out.at[:, :, me, row, :, lane],
            send_sem=out_send.at[c, d],
            recv_sem=out_recv.at[c, d],
            device_id={"energy": peer},
            device_id_type=pl.DeviceIdType.MESH,
        )

    def out_mine(c):
        row, lane = place(c)
        return pltpu.make_async_copy(
            polar_buf.at[c, :, pl.ds(me * kept, kept)], out.at[:, :, me, row, :, lane], out_own.at[c]
        )

    def each(body):
        def step(d, carry):
            body(d)
            return carry
        lax.fori_loop(1, n, step, 0)

    barrier = pltpu.get_barrier_semaphore()
    each(lambda d: pl.semaphore_signal(
        barrier, inc=1, device_id={"energy": lax.rem(me + d, n)}, device_id_type=pl.DeviceIdType.MESH))
    pl.semaphore_wait(barrier, n - 1)

    def send_chunk(c, carry):
        for k in range(2):
            in_own(k, c).start()
            each(lambda d: in_copy(k, c, d).start())
        return carry

    lax.fori_loop(0, chunks, send_chunk, 0)

    def pair(buf, c, i):
        parts = [buf[c, :, :, i + s, :].reshape(2 * count, LANES) for s in range(2)]
        return jnp.concatenate(parts, axis=1)

    def compute_chunk(c, carry):
        for k in range(2):
            in_own(k, c).wait()
            each(lambda d: in_copy(k, c, d).wait_recv())
        for i in range(0, ROWS, 2):
            spec_l = dot(less_tab[...], pair(less_buf, c, i))
            spec_g = dot(great_tab[...], pair(great_buf, c, i))
            half = spec_l.shape[0] // 2
            lr, li, gr, gi = spec_l[:half], spec_l[half:], spec_g[:half], spec_g[half:]
            spec = jnp.concatenate([lr * gr - li * gi, lr * gi + li * gr], axis=0)
            polar = dot(back_tab[...], spec)
            for s in range(2):
                polar_buf[c, :, :, i + s, :] = polar[:, s * LANES:(s + 1) * LANES].reshape(2, keep, LANES)
        out_mine(c).start()
        each(lambda d: out_copy(c, d).start())
        return carry

    lax.fori_loop(0, chunks, compute_chunk, 0)

    def finish(c, carry):
        out_mine(c).wait()
        for k in range(2):
            each(lambda d: in_copy(k, c, d).wait_send())
        each(lambda d: out_copy(c, d).wait())
        return carry

    lax.fori_loop(0, chunks, finish, 0)


def polarization(g_lesser, g_flipped, keep):
    n = lax.axis_size("energy")
    _, held, _, size, width = g_lesser.shape
    count = held * n
    row_parts, lane_parts = size // n // ROWS, width // LANES
    chunks = row_parts * lane_parts
    less = g_lesser.reshape(2, held, n, row_parts, ROWS, width)
    great = g_flipped.reshape(2, held, n, row_parts, ROWS, width)
    tabs = tables(count, keep)
    any_spec = pl.BlockSpec(memory_space=pl.ANY)
    dma = pltpu.SemaphoreType.DMA
    out = pl.pallas_call(
        functools.partial(correlate_kernel, n, lane_parts),
        out_shape=jax.ShapeDtypeStruct((2, keep // n, n, row_parts, ROWS, width), jnp.float32),
        in_specs=[pl.BlockSpec(memory_space=pltpu.VMEM)] * 3 + [any_spec] * 2,
        out_specs=any_spec,
        scratch_shapes=[
            pltpu.VMEM((chunks, 2, count, ROWS, LANES), jnp.float32),
            pltpu.VMEM((chunks, 2, count, ROWS, LANES), jnp.float32),
            pltpu.VMEM((chunks, 2, keep, ROWS, LANES), jnp.float32),
            dma((2, chunks, n)), dma((2, chunks, n)), dma((2, chunks)),
            dma((chunks, n)), dma((chunks, n)), dma((chunks,)),
        ],
        compiler_params=pltpu.CompilerParams(
            collective_id=0, has_side_effects=True, vmem_limit_bytes=56 * 2**20),
    )(*tabs, less, great)
    return out.reshape(2, keep // n, 1, size, width)


def shifted(block, axis, distance):
    devices = range(lax.axis_size(axis))
    return lax.ppermute(block, axis, [(i - distance, i) for i in devices if i - distance in devices])


def sandwich(left, middle, right):
    halfway = jnp.einsum("ab,cwbd->cwad", left, middle, precision=HIGH)
    return jnp.einsum("cwad,df->cwaf", halfway, right, precision=HIGH)


def local(g_lesser, g_greater, v_diag, v_upper):
    polar = polarization(g_lesser, jnp.swapaxes(g_greater, 3, 4), NW)[:, :, 0]
    rows = lax.axis_size("space")
    before = shifted(v_upper, "space", 1)[0]
    diag, upper = v_diag[0], v_upper[0]
    if rows == 2:
        other = lax.ppermute(polar, "space", [(0, 1), (1, 0)])
        coupling = jnp.where(lax.axis_index("space") == 0, upper, before.T)
        total = sandwich(diag, polar, diag) + sandwich(coupling, other, coupling.T)
    else:
        above, below = shifted(polar, "space", 1), shifted(polar, "space", -1)
        total = sandwich(diag, polar, diag)
        total = total + sandwich(before.T, above, before) + sandwich(upper, below, upper.T)
    return total[:, :, None]


def solution(mesh):
    in_specs = (
        P(None, "energy", "space", None, None),
        P(None, "energy", "space", None, None),
        P("space", None, None),
        P("space", None, None),
    )
    out_specs = P(None, "energy", "space", None, None)
    return jax.shard_map(local, mesh=mesh, in_specs=in_specs, out_specs=out_specs, check_vma=False)
```

```python
import functools
import math

import jax
import jax.numpy as jnp
import numpy as np
from jax import lax
from jax.experimental import pallas as pl
from jax.experimental.pallas import tpu as pltpu
from jax.sharding import PartitionSpec as P

NW = 64
PREFACTOR = 0.0625
ROWS = 8
HIGH = lax.Precision.HIGH


def split_np(table):
    table = np.asarray(table, np.float64)
    high = table.astype(jnp.bfloat16)
    low = (table - high.astype(np.float64)).astype(jnp.bfloat16)
    return np.concatenate([high, low, high], axis=1)


def tables(keep):
    length = 2 * keep

    def forward(start, sign):
        phase = 2.0 * math.pi / length * (np.outer(np.arange(length), np.arange(start, start + keep)) % length)
        cos, sin = np.cos(phase), sign * np.sin(phase)
        return np.block([[cos, sin], [-sin, cos]])

    phase = 2.0 * math.pi / length * (np.outer(np.arange(keep), np.arange(length)) % length)
    cos, sin = np.cos(phase) * (PREFACTOR / length), np.sin(phase) * (PREFACTOR / length)
    back = np.block([[cos, -sin], [sin, cos]])
    wide = [np.concatenate([forward(0, sign), forward(keep, sign)], axis=1) for sign in (1, -1)]
    narrow = [forward(0, sign) for sign in (1, -1)]
    return [jnp.asarray(split_np(t)) for t in (*wide, *narrow, back)]


def stacked(value):
    high = value.astype(jnp.bfloat16)
    low = (value - high.astype(jnp.float32)).astype(jnp.bfloat16)
    return jnp.concatenate([high, high, low], axis=0)


def dot(table, value):
    return jnp.dot(table, stacked(value), preferred_element_type=jnp.float32)


def correlate_kernel(
    n, group, less_wide, great_wide, less_narrow, great_narrow, back_tab, less, great, out,
    less_buf, great_buf, halo_buf, polar_buf,
    in_send, in_recv, own_sem, halo_send, halo_recv, out_send, out_recv, out_own,
):
    me = lax.axis_index("energy")
    mine, share = me // group, lax.rem(me, group)
    groups = n // group
    sources, buffers = (less, great), (less_buf, great_buf)
    held = less.shape[1]
    kept = out.shape[2]
    stages = less_buf.shape[0]
    keep = polar_buf.shape[2]
    half = less_buf.shape[4] // 2
    mesh_id = pl.DeviceIdType.MESH

    def in_copy(k, q, d):
        other = lax.rem(share + d, group)
        return pltpu.make_async_remote_copy(
            src_ref=sources[k].at[:, :, other, q],
            dst_ref=buffers[k].at[q, :, pl.ds(share * held, held)],
            send_sem=in_send.at[k, q, d],
            recv_sem=in_recv.at[k, q, d],
            device_id={"energy": mine * group + other},
            device_id_type=mesh_id,
        )

    def in_own(k, q):
        return pltpu.make_async_copy(
            sources[k].at[:, :, share, q], buffers[k].at[q, :, pl.ds(share * held, held)], own_sem.at[k, q]
        )

    def halo_copy(k, q):
        lanes = pl.ds((1 - k) * half, half)
        peer = lax.rem(me + (group if k else n - group), n)
        return pltpu.make_async_remote_copy(
            src_ref=buffers[k].at[q, :, :, :, lanes],
            dst_ref=halo_buf.at[q, :, :, :, lanes],
            send_sem=halo_send.at[k, q],
            recv_sem=halo_recv.at[k, q],
            device_id={"energy": peer},
            device_id_type=mesh_id,
        )

    sends = (mine > 0, mine < groups - 1)
    receives = (mine < groups - 1, mine > 0)

    def out_copy(q, d):
        peer = lax.rem(me + d, n)
        return pltpu.make_async_remote_copy(
            src_ref=polar_buf.at[q, :, pl.ds(peer * kept, kept)],
            dst_ref=out.at[mine, :, :, share, q],
            send_sem=out_send.at[q, d],
            recv_sem=out_recv.at[q, d],
            device_id={"energy": peer},
            device_id_type=mesh_id,
        )

    def out_mine(q):
        return pltpu.make_async_copy(
            polar_buf.at[q, :, pl.ds(me * kept, kept)], out.at[mine, :, :, share, q], out_own.at[q]
        )

    def each(first, last, body):
        def step(d, carry):
            body(d)
            return carry
        lax.fori_loop(first, last, step, 0)

    barrier = pltpu.get_barrier_semaphore()
    each(1, n, lambda d: pl.semaphore_signal(
        barrier, inc=1, device_id={"energy": lax.rem(me + d, n)}, device_id_type=mesh_id))
    pl.semaphore_wait(barrier, n - 1)

    def send_stage(q):
        for k in range(2):
            in_own(k, q).start()
            each(1, group, lambda d: in_copy(k, q, d).start())

    each(0, stages, send_stage)

    def forward_stage(q):
        for k in range(2):
            in_own(k, q).wait()
            each(1, group, lambda d: in_copy(k, q, d).wait_recv())

            @pl.when(sends[k])
            def _():
                halo_copy(k, q).start()

    def pair(buf, q, i, j):
        lanes = slice(j * half, (j + 1) * half)
        return jnp.concatenate([buf[q, :, :, i + s, lanes].reshape(2 * keep, half) for s in range(2)], axis=1)

    def compute_stage(q):
        for k in range(2):
            @pl.when(receives[k])
            def _():
                halo_copy(k, q).wait_recv()

            @pl.when(jnp.logical_not(receives[k]))
            def _():
                lanes = slice((1 - k) * half, (2 - k) * half)
                halo_buf[q, :, :, :, lanes] = jnp.zeros((2, keep, ROWS, half), jnp.float32)

        for i in range(0, ROWS, 2):
            for j in range(2):
                less_x, great_x = pair(less_buf, q, i, j), pair(great_buf, q, i, j)
                halo_x = pair(halo_buf, q, i, j)
                if j == 0:
                    spec_l = dot(less_narrow[...], less_x)
                    spec_g = dot(great_wide[...], jnp.concatenate([great_x, halo_x], axis=0))
                else:
                    spec_l = dot(less_wide[...], jnp.concatenate([less_x, halo_x], axis=0))
                    spec_g = dot(great_narrow[...], great_x)
                mid = spec_l.shape[0] // 2
                lr, li, gr, gi = spec_l[:mid], spec_l[mid:], spec_g[:mid], spec_g[mid:]
                spec = jnp.concatenate([lr * gr - li * gi, lr * gi + li * gr], axis=0)
                polar = dot(back_tab[...], spec)
                for s in range(2):
                    polar_buf[q, :, :, i + s, j * half:(j + 1) * half] = (
                        polar[:, s * half:(s + 1) * half].reshape(2, keep, half))
        out_mine(q).start()
        each(1, n, lambda d: out_copy(q, d).start())

    forward_stage(0)

    def step(q):
        @pl.when(q < stages - 1)
        def _():
            forward_stage(q + 1)
        compute_stage(q)

    each(0, stages, step)

    def finish(q):
        out_mine(q).wait()
        for k in range(2):
            each(1, group, lambda d: in_copy(k, q, d).wait_send())

            @pl.when(sends[k])
            def _():
                halo_copy(k, q).wait_send()
        each(1, n, lambda d: out_copy(q, d).wait())

    each(0, stages, finish)


def polarization(g_lesser, g_flipped, keep):
    n = lax.axis_size("energy")
    _, held, _, size, width = g_lesser.shape
    group = keep // held
    stages = size // group // ROWS
    less = g_lesser.reshape(2, held, group, stages, ROWS, width)
    great = g_flipped.reshape(2, held, group, stages, ROWS, width)
    tabs = tables(keep)
    any_spec = pl.BlockSpec(memory_space=pl.ANY)
    dma = pltpu.SemaphoreType.DMA
    block = pltpu.VMEM((stages, 2, keep, ROWS, width), jnp.float32)
    out = pl.pallas_call(
        functools.partial(correlate_kernel, n, group),
        out_shape=jax.ShapeDtypeStruct((n // group, 2, keep // n, group, stages, ROWS, width), jnp.float32),
        in_specs=[pl.BlockSpec(memory_space=pltpu.VMEM)] * len(tabs) + [any_spec] * 2,
        out_specs=any_spec,
        scratch_shapes=[
            block, block, block, block,
            dma((2, stages, group)), dma((2, stages, group)), dma((2, stages)),
            dma((2, stages)), dma((2, stages)),
            dma((stages, n)), dma((stages, n)), dma((stages,)),
        ],
        compiler_params=pltpu.CompilerParams(
            collective_id=0, has_side_effects=True, vmem_limit_bytes=56 * 2**20),
    )(*tabs, less, great)
    return jnp.sum(out, axis=0).reshape(2, keep // n, 1, size, width)


def shifted(block, axis, distance):
    devices = range(lax.axis_size(axis))
    return lax.ppermute(block, axis, [(i - distance, i) for i in devices if i - distance in devices])


def sandwich(left, middle, right):
    halfway = jnp.einsum("ab,cwbd->cwad", left, middle, precision=HIGH)
    return jnp.einsum("cwad,df->cwaf", halfway, right, precision=HIGH)


def local(g_lesser, g_greater, v_diag, v_upper):
    polar = polarization(g_lesser, jnp.swapaxes(g_greater, 3, 4), NW)[:, :, 0]
    rows = lax.axis_size("space")
    before = shifted(v_upper, "space", 1)[0]
    diag, upper = v_diag[0], v_upper[0]
    if rows == 2:
        other = lax.ppermute(polar, "space", [(0, 1), (1, 0)])
        coupling = jnp.where(lax.axis_index("space") == 0, upper, before.T)
        total = sandwich(diag, polar, diag) + sandwich(coupling, other, coupling.T)
    else:
        above, below = shifted(polar, "space", 1), shifted(polar, "space", -1)
        total = sandwich(diag, polar, diag)
        total = total + sandwich(before.T, above, before) + sandwich(upper, below, upper.T)
    return total[:, :, None]


def solution(mesh):
    in_specs = (
        P(None, "energy", "space", None, None),
        P(None, "energy", "space", None, None),
        P("space", None, None),
        P("space", None, None),
    )
    out_specs = P(None, "energy", "space", None, None)
    return jax.shard_map(local, mesh=mesh, in_specs=in_specs, out_specs=out_specs, check_vma=False)
```
